32 devices in a mesh: seq: 8 (over z, y), head: 4 (over x, core).
Axes of the slice: x: 2, y: 2, z: 4, core: 2. Of those that a mesh axis runs over, the one named last changes fastest.
Arguments:
- image_patches: bfloat16 [8, 256, 1152], P('seq', None, 'head'), may hold values from -6 to 6
- text_embed: bfloat16 [2048, 2048], P('seq', 'head'), may hold values from -6 to 6
- image_start: int32 [8], replicated, may hold values from 0 to 30, as said below
- image_forget: float32 [8], replicated, may hold values from 0.001 to 0.3
- adapter: bfloat16 [1152, 2048], P('head'), may hold values from -0.1875 to 0.1875
- norm_gain: float32 [2048], replicated, may hold values from 0.5 to 1.5
- in_proj: bfloat16 [2048, 4, 2048], P(None, None, 'head'), may hold values from -0.125 to 0.125
- decay_proj: bfloat16 [2048, 16], P(None, 'head'), may hold values from -0.125 to 0.125
- head_decay_ceiling: float32 [16], P('head'), may hold values from 0 to 1, as said below
- out_gain: float32 [16, 128], P('head'), may hold values from 0.5 to 1.5
- out_proj: bfloat16 [2048, 2048], P('head'), may hold values from -0.125 to 0.125
Outputs:
- image_out: bfloat16 [8, 256, 2048], P('seq', None, 'head')
- text_out: bfloat16 [2048, 2048], P('seq', 'head')
The draws below stay inside these ranges and needn't reach their ends.
Inputs may be any that keep to these rules, and one draw needn't show every extreme that they name: `image_start`: each entry is even; the images take distinct pairs of blocks. The merged piece of 512 tokens on one device of seq never holds both the image and the text that one device of seq holds in the source layout. `head_decay_ceiling`: Positive.
All inputs are finite; a program needn't handle non-finite values.
Results may differ from the reference program's by a relative error of at most 0.0095.
Values may be sent and summed in bfloat16 or wider, within the bound.
A program may use at most 128 MiB of HBM per device.

```python
import math
import jax
import jax.numpy as jnp
from jax import lax

H = 16
HD = 128
PIN = 1152
PATCH_COUNT = 256
D = 2048
TOK_DEV = 512
IMAGES = 8
TEXT = 2048
LENGTH = 4096
N_SEQ = 8


def draw_image_start(key, part):
    first_key = jax.random.fold_in(key, 11)
    second_key = jax.random.fold_in(key, 12)
    unit_count = 2 * IMAGES
    shuffled = jax.random.permutation(first_key, unit_count)
    flags = (shuffled < IMAGES).astype(jnp.int32)
    ranking = jnp.argsort((1 - flags) * unit_count + jnp.arange(unit_count, dtype=jnp.int32))
    image_units = ranking[:IMAGES].astype(jnp.int32)
    rotation = 2 * jax.random.randint(second_key, (), 0, IMAGES // 2) + 1
    ordinal = (jnp.arange(IMAGES, dtype=jnp.int32) - rotation) % IMAGES
    return (2 * jnp.take(image_units, ordinal)).astype(jnp.int32)


def draw_head_decay_ceiling(key, part):
    slow_key = jax.random.fold_in(key, 21)
    fast_key = jax.random.fold_in(key, 22)
    pick_key = jax.random.fold_in(key, 23)
    slow = jnp.exp(jax.random.uniform(slow_key, (H,), minval=math.log(0.2 / LENGTH), maxval=math.log(1.5 / LENGTH)))
    fast = jnp.exp(jax.random.uniform(fast_key, (H,), minval=math.log(0.02), maxval=math.log(0.1)))
    share = 0.5
    keeping = jax.random.uniform(pick_key, (H,)) < share
    return jnp.where(keeping, slow, fast).astype(jnp.float32)


def levels(own_key, extent, shards, low, largest):
    gain = 1.0
    for axis_at, shards_of in shards:
        heights = jax.random.uniform(jax.random.fold_in(jax.random.fold_in(own_key, 6), axis_at), (shards_of,), jnp.float32, low / len(shards), largest / len(shards))
        gain = gain * jnp.repeat(jnp.exp(heights), extent[axis_at] // shards_of).reshape((-1,) + (1,) * (len(extent) - 1 - axis_at))
    return gain


def centred(stream_key, extent, spread, bound, shards=(), kind=jnp.bfloat16):
    level = levels(stream_key, extent, shards, -0.22, 0.18) if shards else 1.0
    values = jax.random.normal(stream_key, extent, jnp.float32) * spread * level
    return jnp.minimum(jnp.maximum(values, -bound), bound).astype(kind)


def setup_inputs(seed: int = 0) -> dict:
    streams_of = jax.random.split(jax.random.key(seed), 12)
    return {
        "image_patches": centred(streams_of[0], (IMAGES, PATCH_COUNT, PIN), 1.0, 6.0, ((0, 8), (2, 4))),
        "text_embed": centred(streams_of[1], (TEXT, D), 1.0, 6.0, ((0, 8), (1, 4))),
        "image_start": draw_image_start(jax.random.fold_in(streams_of[11], 71), 0),
        "image_forget": jnp.clip(jnp.exp(jax.random.uniform(streams_of[3], (IMAGES,), jnp.float32, math.log(0.001), math.log(0.3))), 0.001, 0.3),
        "adapter": centred(streams_of[4], (PIN, D), PIN ** -0.5, 0.1875, ((0, 4),)),
        "norm_gain": jnp.clip(1.0 + 0.1 * jax.random.normal(streams_of[5], (D,), jnp.float32), 0.5, 1.5),
        "in_proj": centred(streams_of[6], (D, 4, D), D ** -0.5, 0.125, ((2, 4),)),
        "decay_proj": centred(streams_of[7], (D, H), D ** -0.5, 0.125, ((1, 4),)),
        "head_decay_ceiling": draw_head_decay_ceiling(jax.random.fold_in(streams_of[11], 71), 0),
        "out_gain": jnp.clip(1.0 + 0.1 * jax.random.normal(streams_of[9], (H, HD), jnp.float32), 0.5, 1.5),
        "out_proj": centred(streams_of[10], (D, D), D ** -0.5, 0.125, ((0, 4),)),
    }


EPSILON = 1e-06

def rms_scale(values, gain_row):
    mean_square = lax.optimization_barrier(jnp.mean(values * values, axis=-1, keepdims=True))
    return values * lax.rsqrt(mean_square + EPSILON) * gain_row

def group_step(state_in, inputs):
    queries, key_rows, value_rows, decay_logarithm = inputs
    row_count = queries.shape[0]
    within = jnp.cumsum(decay_logarithm, axis=0)
    span_decay = within[-1]
    query_f = queries.astype(jnp.float32)
    key_f = key_rows.astype(jnp.float32)
    value_f = value_rows.astype(jnp.float32)
    scores = jnp.einsum('thd,shd->hts', query_f, key_f)
    lagged = within.T[:, :, None] - within.T[:, None, :]
    row_ids = jnp.arange(row_count, dtype=jnp.int32)
    causal = (row_ids[:, None] >= row_ids[None, :])[None]
    weights = jnp.where(causal, scores * jnp.exp(jnp.where(causal, lagged, 0.0)), 0.0).astype(jnp.bfloat16)
    inner_part = jnp.einsum('hts,shd->thd', weights.astype(jnp.float32), value_f)
    carried = jnp.exp(within)[:, :, None] * jnp.einsum('thd,hde->the', query_f, state_in, precision=lax.Precision.HIGHEST)
    weighted_keys = key_f * jnp.exp(span_decay[None, :] - within)[:, :, None]
    local_state = jnp.einsum('thd,the->hde', weighted_keys, value_f, precision=lax.Precision.HIGHEST)
    new_state = jnp.exp(span_decay)[:, None, None] * state_in + local_state
    return (new_state, inner_part + carried)

def by_device(values):
    return values.reshape((N_SEQ, TOK_DEV) + values.shape[1:])

def reference(image_patches, text_embed, image_start, image_forget, adapter, norm_gain, in_proj, decay_proj, head_decay_ceiling, out_gain, out_proj):
    unit_count = 2 * IMAGES
    image_rows = jnp.dot(image_patches.reshape(IMAGES * PATCH_COUNT, PIN), adapter, preferred_element_type=jnp.float32)
    image_embed = image_rows.astype(jnp.bfloat16).reshape(IMAGES, PATCH_COUNT, D)
    unit_of_image = (image_start // 2).astype(jnp.int32)
    unit_ids = jnp.arange(unit_count, dtype=jnp.int32)
    image_ids = jnp.arange(IMAGES, dtype=jnp.int32)
    image_hits = (unit_of_image[:, None] == unit_ids[None, :]).astype(jnp.int32)
    is_image = lax.optimization_barrier(jnp.sum(image_hits, axis=0)).astype(jnp.int32)
    image_here = lax.optimization_barrier(jnp.sum(image_hits * image_ids[:, None], axis=0)).astype(jnp.int32)
    is_text = (1 - is_image).astype(jnp.int32)
    text_here = (jnp.cumsum(is_text) - is_text).astype(jnp.int32)
    source = jnp.where(is_image == 1, image_here, IMAGES + text_here).astype(jnp.int32)
    pieces = jnp.concatenate([image_embed, text_embed.reshape(IMAGES, PATCH_COUNT, D)], axis=0)
    merged = jnp.take(pieces, source, axis=0).reshape(LENGTH, D)
    forget_element = jnp.where(is_image == 1, jnp.log1p(-jnp.take(image_forget, image_here)), 0.0)
    start_offsets = jnp.arange(LENGTH, dtype=jnp.int32) % PATCH_COUNT == 0
    surge_logarithm = jnp.where(start_offsets, jnp.repeat(forget_element, PATCH_COUNT), 0.0)
    normed = rms_scale(merged.astype(jnp.float32), norm_gain).astype(jnp.bfloat16)
    projected = jnp.dot(normed, in_proj.reshape(D, 4 * D), preferred_element_type=jnp.float32)
    projected = projected.astype(jnp.bfloat16).reshape(LENGTH, 4, H, HD)
    gate_preactivation = jnp.dot(normed, decay_proj, preferred_element_type=jnp.float32)
    decay_logarithm = -head_decay_ceiling[None, :] * jax.nn.sigmoid(gate_preactivation) + surge_logarithm[:, None]
    start_state = jnp.zeros((H, HD, HD), jnp.float32)
    last_state, attended = lax.scan(group_step, start_state, (by_device(projected[:, 0]), by_device(projected[:, 1]), by_device(projected[:, 2]), by_device(decay_logarithm)))
    attended = attended.reshape(LENGTH, H, HD)
    gated = rms_scale(attended, out_gain) * jax.nn.silu(projected[:, 3].astype(jnp.float32))
    gated = gated.astype(jnp.bfloat16).reshape(LENGTH, D)
    result = (merged.astype(jnp.float32) + jnp.dot(gated, out_proj, preferred_element_type=jnp.float32)).astype(jnp.bfloat16)
    out_units = result.reshape(unit_count, PATCH_COUNT, D)
    image_out = jnp.take(out_units, unit_of_image, axis=0)
    text_pick = ((is_text[None, :] == 1) & (text_here[None, :] == image_ids[:, None])).astype(jnp.int32)
    text_unit = lax.optimization_barrier(jnp.sum(text_pick * unit_ids[None, :], axis=1)).astype(jnp.int32)
    text_out = jnp.take(out_units, text_unit, axis=0).reshape(TEXT, D)
    return (image_out, text_out)
```

```python
import jax
import jax.numpy as jnp
from jax import lax
from jax.sharding import PartitionSpec as P

EPSILON = 1e-06


def rms_scale(values, gain_row):
    mean_square = jnp.mean(values * values, axis=-1, keepdims=True)
    return values * lax.rsqrt(mean_square + EPSILON) * gain_row


def unit_places(image_start, seq_count):
    unit_ids = jnp.arange(2 * seq_count, dtype=jnp.int32)
    device_ids = jnp.arange(seq_count, dtype=jnp.int32)
    unit_of_image = image_start // 2
    is_text = 1 - jnp.sum(
        (unit_of_image[:, None] == unit_ids[None, :]).astype(jnp.int32), axis=0
    )
    before = (unit_ids[None, :] < unit_ids[:, None]).astype(jnp.int32)
    text_here = jnp.sum(before * is_text[None, :], axis=1)
    text_pick = (is_text[None, :] == 1) & (text_here[None, :] == device_ids[:, None])
    text_unit = jnp.sum(text_pick.astype(jnp.int32) * unit_ids[None, :], axis=1)
    return jnp.stack([unit_of_image, text_unit], axis=1)


def shards(
    image_patches,
    text_embed,
    image_start,
    image_forget,
    adapter,
    norm_gain,
    in_proj,
    decay_proj,
    head_decay_ceiling,
    out_gain,
    out_proj,
):
    seq_count = lax.axis_size("seq")
    me = lax.axis_index("seq")
    rows = text_embed.shape[0]
    model_width = in_proj.shape[0]
    heads = head_decay_ceiling.shape[0]
    head_width = out_gain.shape[1]
    places = unit_places(image_start, seq_count)
    partial_value = jnp.dot(image_patches[0], adapter, preferred_element_type=jnp.float32)
    embedded = lax.psum_scatter(
        partial_value.astype(jnp.bfloat16), "head", scatter_dimension=1, tiled=True
    )
    merged = jnp.concatenate([embedded, text_embed], axis=0)
    full_rows = lax.all_gather(merged, "head", axis=1, tiled=True)
    normed = rms_scale(full_rows.astype(jnp.float32), norm_gain).astype(jnp.bfloat16)
    projected = jnp.dot(
        normed, in_proj.reshape(model_width, -1), preferred_element_type=jnp.float32
    )
    projected = projected.astype(jnp.bfloat16).reshape(2, rows, 4, heads, head_width)
    preact = jnp.dot(normed, decay_proj, preferred_element_type=jnp.float32)
    burst = jnp.log1p(-lax.dynamic_index_in_dim(image_forget, me, 0, False))
    first = jnp.arange(2 * rows, dtype=jnp.int32) == 0
    decay = -head_decay_ceiling[None, :] * jax.nn.sigmoid(preact)
    decay = (decay + jnp.where(first, burst, 0.0)[:, None]).reshape(2, rows, heads)
    queries, keys, values, gates = (projected[:, :, i] for i in range(4))
    within = jnp.cumsum(decay, axis=1)
    span = within[:, -1]
    scores = jnp.einsum("uthd,ushd->uhts", queries, keys, preferred_element_type=jnp.float32)
    across = within.transpose(0, 2, 1)
    lagged = across[:, :, :, None] - across[:, :, None, :]
    row_ids = jnp.arange(rows, dtype=jnp.int32)
    causal = row_ids[:, None] >= row_ids[None, :]
    weights = jnp.where(causal, scores * jnp.exp(jnp.where(causal, lagged, 0.0)), 0.0).astype(
        jnp.bfloat16
    )
    inner = jnp.einsum("uhts,ushd->uthd", weights, values, preferred_element_type=jnp.float32)
    weighted = keys.astype(jnp.float32) * jnp.exp(span[:, None] - within)[..., None]
    state = jnp.einsum(
        "uthd,uthe->uhde",
        weighted.astype(jnp.bfloat16),
        values,
        preferred_element_type=jnp.float32,
    )
    all_state = lax.all_gather(state.astype(jnp.bfloat16), "seq")
    all_span = lax.all_gather(span, "seq")
    mine = lax.dynamic_index_in_dim(places, me, 0, False)
    flat = places.reshape(-1)
    earlier = flat[None, :] < mine[:, None]
    between = earlier[:, None, :] & (flat[None, None, :] > flat[None, :, None])
    passed = jnp.sum(
        jnp.where(between[..., None], all_span.reshape(1, 1, 2 * seq_count, heads), 0.0), axis=2
    )
    share = jnp.where(earlier[..., None], jnp.exp(passed), 0.0)
    entering = jnp.sum(
        share[..., None, None]
        * all_state.reshape(1, 2 * seq_count, heads, head_width, head_width).astype(jnp.float32),
        axis=1,
    )
    carried = jnp.exp(within)[..., None] * jnp.einsum(
        "uthd,uhde->uthe",
        queries,
        entering.astype(jnp.bfloat16),
        preferred_element_type=jnp.float32,
    )
    attended = inner + carried
    gated = rms_scale(attended, out_gain) * jax.nn.silu(gates.astype(jnp.float32))
    gated = gated.astype(jnp.bfloat16).reshape(2 * rows, -1)
    partial_out = jnp.dot(gated, out_proj, preferred_element_type=jnp.float32)
    summed = lax.psum_scatter(
        partial_out.astype(jnp.bfloat16), "head", scatter_dimension=1, tiled=True
    ).astype(jnp.float32)
    result = (merged.astype(jnp.float32) + summed).astype(jnp.bfloat16)
    return (result[:rows][None], result[rows:])


def solution(mesh):
    in_specs = (
        P("seq", None, "head"),
        P("seq", "head"),
        P(),
        P(),
        P("head", None),
        P(),
        P(None, None, "head"),
        P(None, "head"),
        P("head"),
        P("head", None),
        P("head", None),
    )
    out_specs = (P("seq", None, "head"), P("seq", "head"))
    return jax.shard_map(shards, mesh=mesh, in_specs=in_specs, out_specs=out_specs, check_vma=False)
```

```python
import functools

import jax
import jax.numpy as jnp
from jax import lax
from jax.experimental import pallas as pl
from jax.experimental.pallas import tpu as pltpu
from jax.sharding import PartitionSpec as P

EPSILON = 1e-06
LANES = 128
SPAN_ROWS = 8
BF16 = jnp.bfloat16
F32 = jnp.float32


def unit_places(image_start, seq_count):
    unit_ids = jnp.arange(2 * seq_count, dtype=jnp.int32)
    device_ids = jnp.arange(seq_count, dtype=jnp.int32)
    unit_of_image = image_start // 2
    is_text = 1 - jnp.sum(
        (unit_of_image[:, None] == unit_ids[None, :]).astype(jnp.int32), axis=0
    )
    before = (unit_ids[None, :] < unit_ids[:, None]).astype(jnp.int32)
    text_here = jnp.sum(before * is_text[None, :], axis=1)
    text_pick = (is_text[None, :] == 1) & (text_here[None, :] == device_ids[:, None])
    text_unit = jnp.sum(text_pick.astype(jnp.int32) * unit_ids[None, :], axis=1)
    return jnp.stack([unit_of_image, text_unit], axis=1)


def dot(a, b):
    return jnp.dot(a, b, preferred_element_type=F32)


def exact_dot(a, b):
    return jnp.dot(a, b, preferred_element_type=F32, precision=lax.Precision.HIGHEST)


def iota(shape, dim):
    return lax.broadcasted_iota(jnp.int32, shape, dim)


def layer_kernel(
    n,
    heads,
    patches_ref,
    text_ref,
    adapter_ref,
    gain_ref,
    decay_ref,
    ceiling_ref,
    burst_ref,
    out_gain_ref,
    place_row_ref,
    place_col_ref,
    in_proj_ref,
    out_proj_ref,
    image_out_ref,
    text_out_ref,
    w_in,
    w_out,
    gath,
    normed,
    proj,
    inner,
    within_keep,
    half_send,
    half_recv,
    own,
    cross_send,
    cross_recv,
    out_send,
    out_recv,
    out_cross_send,
    out_cross_recv,
    out_own,
    state,
    state_recv,
    entering_send,
    entering,
    span_send,
    span_recv,
    load_sem,
    pair_send_sem,
    pair_recv_sem,
    state_send_sem,
    state_recv_sem,
    span_send_sem,
    span_recv_sem,
    enter_send_sem,
    enter_recv_sem,
    keep_sem,
):
    me = lax.axis_index("seq")
    h = lax.axis_index("head")
    h1 = h + 1 - 2 * lax.rem(h, 2)
    h2 = lax.rem(h + 2, 4)
    h3 = lax.rem(h1 + 2, 4)
    rows, width = text_ref.shape
    part = heads * LANES // n
    in_load = pltpu.make_async_copy(in_proj_ref, w_in, load_sem.at[0])
    out_load = pltpu.make_async_copy(out_proj_ref, w_out, load_sem.at[1])
    in_load.start()
    out_load.start()

    barrier = pltpu.get_barrier_semaphore()
    pl.semaphore_signal(barrier, inc=1, device_id={"head": h1})
    pl.semaphore_signal(barrier, inc=1, device_id={"head": h2})
    for j in range(1, n):
        pl.semaphore_signal(barrier, inc=1, device_id={"seq": lax.rem(me + j, n)})
    pl.semaphore_wait(barrier, n + 1)

    sent = []

    def send(src, dst, index, to):
        copy = pltpu.make_async_remote_copy(
            src_ref=src,
            dst_ref=dst,
            send_sem=pair_send_sem.at[index],
            recv_sem=pair_recv_sem.at[index],
            device_id={"head": to},
        )
        copy.start()
        sent.append(copy)
        return copy

    def columns(block):
        return pl.ds(pl.multiple_of(block * width, width), width)

    text_cross = send(text_ref, gath.at[1, h], 0, h2)
    text_pair = send(text_ref, gath.at[1, h], 1, h1)
    gath[1, h] = text_ref[...]

    half_send[0] = dot(patches_ref[...], adapter_ref[:, columns(h1)]).astype(BF16)
    half_send[1] = dot(patches_ref[...], adapter_ref[:, columns(h3)]).astype(BF16)
    half = send(half_send, half_recv, 2, h1)
    far = dot(patches_ref[...], adapter_ref[:, columns(h2)])
    own[...] = dot(patches_ref[...], adapter_ref[:, columns(h)])
    half.wait_recv()
    cross_send[...] = (far + half_recv[1].astype(F32)).astype(BF16)
    cross = send(cross_send, cross_recv, 3, h2)
    own[...] = own[...] + half_recv[0].astype(F32)

    text_cross.wait_recv()
    text_relay = send(gath.at[1, h2], gath.at[1, h2], 4, h1)
    text_pair.wait_recv()
    text_relay.wait_recv()

    def project(k):
        blocks = [gath[k, b].astype(F32) for b in range(4)]
        square = sum(jnp.sum(x * x, axis=1, keepdims=True) for x in blocks)
        scale = lax.rsqrt(square / (4 * width) + EPSILON)
        for b in range(4):
            gain = gain_ref[:, b * width : (b + 1) * width]
            normed[:, b * width : (b + 1) * width] = (blocks[b] * scale * gain).astype(BF16)
        for q in range(4):
            proj[k, q] = dot(normed[...], w_in[:, q * width : (q + 1) * width]).astype(BF16)
        preact = dot(normed[...], decay_ref[...])
        decay = -ceiling_ref[...] * jax.nn.sigmoid(preact)
        if k == 0:
            decay = decay + jnp.where(iota(decay.shape, 0) == 0, burst_ref[...], 0.0)
        lower = (iota((rows, rows), 0) >= iota((rows, rows), 1)).astype(F32)
        within = exact_dot(lower, decay)
        within_keep[k] = within
        span_send[k : k + 1, :] = within[rows - 1 :, :]

    def attend(k):
        within = within_keep[k]
        across = within.T
        tail = jnp.exp(within[rows - 1 :, :] - within)
        causal = iota((rows, rows), 0) >= iota((rows, rows), 1)
        for i in range(heads):
            lane = slice(i * LANES, (i + 1) * LANES)
            query, key, value = (proj[k, q, :, lane] for q in range(3))
            scores = lax.dot_general(
                query, key, (((1,), (1,)), ((), ())), preferred_element_type=F32
            )
            lagged = within[:, i : i + 1] - across[i : i + 1, :]
            fade = jnp.exp(jnp.where(causal, lagged, 0.0))
            weights = jnp.where(causal, scores * fade, 0.0).astype(BF16)
            inner[k, :, lane] = dot(weights, value)
            weighted = key.astype(F32) * tail[:, i : i + 1]
            state[k, lane, :] = dot(weighted.T.astype(BF16), value).astype(BF16)

    span_send[...] = jnp.zeros_like(span_send)
    in_load.wait()
    project(1)

    cross.wait_recv()
    gath[0, h] = (own[...] + cross_recv[...].astype(F32)).astype(BF16)
    image_cross = send(gath.at[0, h], gath.at[0, h], 5, h2)
    image_pair = send(gath.at[0, h], gath.at[0, h], 6, h1)
    attend(1)
    image_cross.wait_recv()
    image_relay = send(gath.at[0, h2], gath.at[0, h2], 7, h1)
    image_pair.wait_recv()
    image_relay.wait_recv()
    project(0)

    def spread(source, target, send_sem, recv_sem):
        copies = []
        for j in range(1, n):
            peer = lax.rem(me + j, n)
            copy = pltpu.make_async_remote_copy(
                src_ref=source(peer),
                dst_ref=target,
                send_sem=send_sem.at[j],
                recv_sem=recv_sem.at[j],
                device_id={"seq": peer},
            )
            copy.start()
            copies.append(copy)
        sent.extend(copies)
        return copies

    def piece(device):
        return pl.ds(pl.multiple_of(device * part, part), part)

    spans = spread(lambda peer: span_send, span_recv.at[me], span_send_sem, span_recv_sem)
    span_recv[me] = span_send[...]
    attend(0)
    states = spread(
        lambda peer: state.at[:, piece(peer)], state_recv.at[me], state_send_sem, state_recv_sem
    )
    keep_state = pltpu.make_async_copy(state.at[:, piece(me)], state_recv.at[me], keep_sem.at[0])
    keep_state.start()

    for copy in spans:
        copy.wait_recv()
    units = SPAN_ROWS * n
    my_head = (me * part) // LANES
    table = span_recv[...].reshape(units, LANES)
    span_col = jnp.sum(
        jnp.where(iota(table.shape, 1) == my_head, table, 0.0), axis=1, keepdims=True
    )
    eye = iota((units, units), 0) == iota((units, units), 1)
    span_row = jnp.sum(jnp.where(eye, span_col, 0.0), axis=0, keepdims=True)
    place_row, place_col = place_row_ref[...], place_col_ref[...]
    earlier = place_row < place_col
    later = place_col < place_row
    begin_col = jnp.sum(jnp.where(earlier, span_row, 0.0), axis=1, keepdims=True)
    begin_row = jnp.sum(jnp.where(later, span_col, 0.0), axis=0, keepdims=True)
    passed = jnp.minimum(begin_col - begin_row - span_row, 0.0)
    share = jnp.where(earlier, jnp.exp(passed), 0.0)
    share_high = share.astype(BF16)
    share_low = (share - share_high.astype(F32)).astype(BF16)
    total = 2 * n * part

    def unit_of(index):
        return index // (2 * part) * SPAN_ROWS + (index // part) % 2

    tall = (unit_of(iota((total, units), 0)) == iota((total, units), 1)).astype(BF16)
    wide = (unit_of(iota((units, total), 1)) == iota((units, total), 0)).astype(BF16)
    same = iota((total, total), 0) % part == iota((total, total), 1) % part

    def expand(values):
        grid = dot(dot(tall, values).astype(BF16), wide)
        return jnp.where(same, grid, 0.0).astype(BF16)

    mix_high = expand(share_high)
    mix_low = expand(share_low)
    keep_state.wait()
    for copy in states:
        copy.wait_recv()
    every = state_recv[...].reshape(total, LANES)
    joined = dot(mix_high, every) + dot(mix_low, every)
    entering_send[...] = joined.astype(BF16).reshape(n, 2, part, LANES)
    enters = spread(
        lambda peer: entering_send.at[peer],
        entering.at[:, piece(me)],
        enter_send_sem,
        enter_recv_sem,
    )
    keep_enter = pltpu.make_async_copy(
        entering_send.at[me], entering.at[:, piece(me)], keep_sem.at[1]
    )
    keep_enter.start()
    out_load.wait()
    keep_enter.wait()
    for copy in enters:
        copy.wait_recv()

    def finish(k):
        grown = jnp.exp(within_keep[k])
        pieces = []
        for i in range(heads):
            lane = slice(i * LANES, (i + 1) * LANES)
            carried = grown[:, i : i + 1] * dot(proj[k, 0, :, lane], entering[k, lane, :])
            attended = inner[k, :, lane] + carried
            mean_square = jnp.mean(attended * attended, axis=1, keepdims=True)
            unit = attended * lax.rsqrt(mean_square + EPSILON) * out_gain_ref[i : i + 1, :]
            gate = proj[k, 3, :, lane].astype(F32)
            pieces.append((unit * gate * jax.nn.sigmoid(gate)).astype(BF16))
        gated = jnp.concatenate(pieces, axis=1)
        out_send[k, 0] = dot(gated, w_out[:, columns(h3)]).astype(BF16)
        out_send[k, 1] = dot(gated, w_out[:, columns(h1)]).astype(BF16)
        copy = send(out_send.at[k], out_recv.at[k], 8 + k, h1)
        distant = dot(gated, w_out[:, columns(h2)])
        out_own[k] = dot(gated, w_out[:, columns(h)])
        copy.wait_recv()
        out_cross_send[k] = (distant + out_recv[k, 0].astype(F32)).astype(BF16)
        return send(out_cross_send.at[k], out_cross_recv.at[k], 10 + k, h2)

    def result(k):
        total_out = out_own[k] + out_recv[k, 1].astype(F32) + out_cross_recv[k].astype(F32)
        return (gath[k, h].astype(F32) + total_out).astype(BF16)

    first = finish(0)
    second = finish(1)
    first.wait_recv()
    image_out_ref[0] = result(0)
    second.wait_recv()
    text_out_ref[...] = result(1)
    for copy in sent:
        copy.wait_send()


def shards(
    image_patches,
    text_embed,
    image_start,
    image_forget,
    adapter,
    norm_gain,
    in_proj,
    decay_proj,
    head_decay_ceiling,
    out_gain,
    out_proj,
):
    n = lax.axis_size("seq")
    me = lax.axis_index("seq")
    rows, width = text_embed.shape
    model_width = in_proj.shape[0]
    heads = head_decay_ceiling.shape[0]
    part = heads * LANES // n
    places = unit_places(image_start, n)
    places = jnp.pad(places, ((0, 0), (0, SPAN_ROWS - 2)), constant_values=0).reshape(-1)
    used = jnp.arange(SPAN_ROWS * n) % SPAN_ROWS < 2
    place_row = jnp.where(used, places, 4 * n)[None, :]
    place_col = jnp.where(used, places, 4 * n)[:, None]
    burst = jnp.log1p(-lax.dynamic_index_in_dim(image_forget, me, 0, True))
    burst = jnp.broadcast_to(burst[None, :], (1, LANES))
    decay_pad = jnp.pad(decay_proj, ((0, 0), (0, LANES - heads)))
    ceiling = jnp.pad(head_decay_ceiling, (0, LANES - heads))[None, :]
    vmem = pl.BlockSpec(memory_space=pltpu.VMEM)
    hbm = pl.BlockSpec(memory_space=pl.ANY)
    dma = pltpu.SemaphoreType.DMA
    return pl.pallas_call(
        functools.partial(layer_kernel, n, heads),
        out_shape=(
            jax.ShapeDtypeStruct((1, rows, width), BF16),
            jax.ShapeDtypeStruct((rows, width), BF16),
        ),
        in_specs=[vmem] * 10 + [hbm] * 2,
        out_specs=(vmem, vmem),
        scratch_shapes=[
            pltpu.VMEM((model_width, 4 * width), BF16),
            pltpu.VMEM((width, model_width), BF16),
            pltpu.VMEM((2, 4, rows, width), BF16),
            pltpu.VMEM((rows, model_width), BF16),
            pltpu.VMEM((2, 4, rows, width), BF16),
            pltpu.VMEM((2, rows, width), F32),
            pltpu.VMEM((2, rows, LANES), F32),
            pltpu.VMEM((2, rows, width), BF16),
            pltpu.VMEM((2, rows, width), BF16),
            pltpu.VMEM((rows, width), F32),
            pltpu.VMEM((rows, width), BF16),
            pltpu.VMEM((rows, width), BF16),
            pltpu.VMEM((2, 2, rows, width), BF16),
            pltpu.VMEM((2, 2, rows, width), BF16),
            pltpu.VMEM((2, rows, width), BF16),
            pltpu.VMEM((2, rows, width), BF16),
            pltpu.VMEM((2, rows, width), F32),
            pltpu.VMEM((2, heads * LANES, LANES), BF16),
            pltpu.VMEM((n, 2, part, LANES), BF16),
            pltpu.VMEM((n, 2, part, LANES), BF16),
            pltpu.VMEM((2, heads * LANES, LANES), BF16),
            pltpu.VMEM((SPAN_ROWS, LANES), F32),
            pltpu.VMEM((n, SPAN_ROWS, LANES), F32),
            dma((2,)),
            dma((12,)),
            dma((12,)),
            dma((n,)),
            dma((n,)),
            dma((n,)),
            dma((n,)),
            dma((n,)),
            dma((n,)),
            dma((2,)),
        ],
        compiler_params=pltpu.CompilerParams(
            collective_id=0, has_side_effects=True, vmem_limit_bytes=60 * 1024 * 1024
        ),
    )(
        image_patches[0],
        text_embed,
        adapter,
        norm_gain[None, :],
        decay_pad,
        ceiling,
        burst,
        out_gain,
        place_row,
        place_col,
        in_proj.reshape(model_width, -1),
        out_proj,
    )


def solution(mesh):
    in_specs = (
        P("seq", None, "head"),
        P("seq", "head"),
        P(),
        P(),
        P("head", None),
        P(),
        P(None, None, "head"),
        P(None, "head"),
        P("head"),
        P("head", None),
        P("head", None),
    )
    out_specs = (P("seq", None, "head"), P("seq", "head"))
    return jax.shard_map(shards, mesh=mesh, in_specs=in_specs, out_specs=out_specs, check_vma=False)
```

```python
import functools

import jax
import jax.numpy as jnp
from jax import lax
from jax.experimental import pallas as pl
from jax.experimental.pallas import tpu as pltpu
from jax.sharding import PartitionSpec as P

EPSILON = 1e-06
LANES = 128
SPAN_ROWS = 8
BF16 = jnp.bfloat16
F32 = jnp.float32


def unit_places(image_start, seq_count):
    unit_ids = jnp.arange(2 * seq_count, dtype=jnp.int32)
    device_ids = jnp.arange(seq_count, dtype=jnp.int32)
    unit_of_image = image_start // 2
    is_text = 1 - jnp.sum(
        (unit_of_image[:, None] == unit_ids[None, :]).astype(jnp.int32), axis=0
    )
    before = (unit_ids[None, :] < unit_ids[:, None]).astype(jnp.int32)
    text_here = jnp.sum(before * is_text[None, :], axis=1)
    text_pick = (is_text[None, :] == 1) & (text_here[None, :] == device_ids[:, None])
    text_unit = jnp.sum(text_pick.astype(jnp.int32) * unit_ids[None, :], axis=1)
    return jnp.stack([unit_of_image, text_unit], axis=1)


def dot(a, b):
    return jnp.dot(a, b, preferred_element_type=F32)


def exact_dot(a, b):
    return jnp.dot(a, b, preferred_element_type=F32, precision=lax.Precision.HIGHEST)


def iota(shape, dim):
    return lax.broadcasted_iota(jnp.int32, shape, dim)


def layer_kernel(
    n,
    heads,
    patches_ref,
    text_ref,
    adapter_ref,
    gain_ref,
    decay_ref,
    ceiling_ref,
    burst_ref,
    out_gain_ref,
    place_row_ref,
    place_col_ref,
    in_proj_ref,
    out_proj_ref,
    image_out_ref,
    text_out_ref,
    w_raw,
    w_flat,
    w_in,
    w_out,
    gath,
    normed,
    proj,
    inner,
    within_keep,
    half_send,
    half_recv,
    own,
    cross_send,
    cross_recv,
    out_send,
    out_recv,
    out_cross_send,
    out_cross_recv,
    out_own,
    state,
    state_recv,
    entering_send,
    entering,
    span_send,
    span_recv,
    load_sem,
    pair_send_sem,
    pair_recv_sem,
    state_send_sem,
    state_recv_sem,
    span_send_sem,
    span_recv_sem,
    enter_send_sem,
    enter_recv_sem,
    keep_sem,
):
    me = lax.axis_index("seq")
    h = lax.axis_index("head")
    h1 = h + 1 - 2 * lax.rem(h, 2)
    h2 = lax.rem(h + 2, 4)
    h3 = lax.rem(h1 + 2, 4)
    rows, width = text_ref.shape
    part = heads * LANES // n
    in_load = pltpu.make_async_copy(in_proj_ref.reshape(4 * in_proj_ref.shape[0], width), w_raw, load_sem.at[0])
    out_load = pltpu.make_async_copy(out_proj_ref, w_out, load_sem.at[1])
    in_load.start()
    out_load.start()

    barrier = pltpu.get_barrier_semaphore()
    pl.semaphore_signal(barrier, inc=1, device_id={"head": h1})
    pl.semaphore_signal(barrier, inc=1, device_id={"head": h2})
    for j in range(1, n):
        pl.semaphore_signal(barrier, inc=1, device_id={"seq": lax.rem(me + j, n)})
    pl.semaphore_wait(barrier, n + 1)

    sent = []

    def send(src, dst, index, to):
        copy = pltpu.make_async_remote_copy(
            src_ref=src,
            dst_ref=dst,
            send_sem=pair_send_sem.at[index],
            recv_sem=pair_recv_sem.at[index],
            device_id={"head": to},
        )
        copy.start()
        sent.append(copy)
        return copy

    def columns(block):
        return pl.ds(pl.multiple_of(block * width, width), width)

    text_cross = send(text_ref, gath.at[1, h], 0, h2)
    text_pair = send(text_ref, gath.at[1, h], 1, h1)
    gath[1, h] = text_ref[...]

    half_send[0] = dot(patches_ref[...], adapter_ref[:, columns(h1)]).astype(BF16)
    half_send[1] = dot(patches_ref[...], adapter_ref[:, columns(h3)]).astype(BF16)
    half = send(half_send, half_recv, 2, h1)
    far = dot(patches_ref[...], adapter_ref[:, columns(h2)])
    own[...] = dot(patches_ref[...], adapter_ref[:, columns(h)])
    half.wait_recv()
    cross_send[...] = (far + half_recv[1].astype(F32)).astype(BF16)
    cross = send(cross_send, cross_recv, 3, h2)
    own[...] = own[...] + half_recv[0].astype(F32)

    in_load.wait()
    step_rows = 128

    @pl.loop(0, w_in.shape[1] // step_rows)
    def _(step):
        flat = w_raw[pl.ds(pl.multiple_of(step * 512, 512), 512), :].astype(F32)
        for b in range(width // LANES):
            w_flat[b] = flat[:, b * LANES : (b + 1) * LANES]
        for q in range(4):
            for c in range(step_rows // 64):
                taken = jnp.concatenate(
                    [
                        w_flat[b, pl.ds(c * 256 + q, 64, stride=4), :]
                        for b in range(width // LANES)
                    ],
                    axis=1,
                )
                base = pl.multiple_of(step * step_rows + c * 64, 64)
                w_in[q, pl.ds(base, 64), :] = taken.astype(BF16)

    text_cross.wait_recv()
    text_relay = send(gath.at[1, h2], gath.at[1, h2], 4, h1)
    text_pair.wait_recv()
    text_relay.wait_recv()

    def project(k):
        blocks = [gath[k, b].astype(F32) for b in range(4)]
        square = sum(jnp.sum(x * x, axis=1, keepdims=True) for x in blocks)
        scale = lax.rsqrt(square / (4 * width) + EPSILON)
        for b in range(4):
            gain = gain_ref[:, b * width : (b + 1) * width]
            normed[:, b * width : (b + 1) * width] = (blocks[b] * scale * gain).astype(BF16)
        for q in range(4):
            proj[k, q] = dot(normed[...], w_in[q]).astype(BF16)
        preact = dot(normed[...], decay_ref[...])
        decay = -ceiling_ref[...] * jax.nn.sigmoid(preact)
        if k == 0:
            decay = decay + jnp.where(iota(decay.shape, 0) == 0, burst_ref[...], 0.0)
        lower = (iota((rows, rows), 0) >= iota((rows, rows), 1)).astype(F32)
        within = exact_dot(lower, decay)
        within_keep[k] = within
        span_send[k : k + 1, :] = within[rows - 1 :, :]

    def attend(k):
        within = within_keep[k]
        across = within.T
        tail = jnp.exp(within[rows - 1 :, :] - within)
        causal = iota((rows, rows), 0) >= iota((rows, rows), 1)
        for i in range(heads):
            lane = slice(i * LANES, (i + 1) * LANES)
            query, key, value = (proj[k, q, :, lane] for q in range(3))
            scores = lax.dot_general(
                query, key, (((1,), (1,)), ((), ())), preferred_element_type=F32
            )
            lagged = within[:, i : i + 1] - across[i : i + 1, :]
            fade = jnp.exp(jnp.where(causal, lagged, 0.0))
            weights = jnp.where(causal, scores * fade, 0.0).astype(BF16)
            inner[k, :, lane] = dot(weights, value)
            weighted = key.astype(F32) * tail[:, i : i + 1]
            state[k, lane, :] = dot(weighted.T.astype(BF16), value).astype(BF16)

    span_send[...] = jnp.zeros_like(span_send)
    project(1)

    cross.wait_recv()
    gath[0, h] = (own[...] + cross_recv[...].astype(F32)).astype(BF16)
    image_cross = send(gath.at[0, h], gath.at[0, h], 5, h2)
    image_pair = send(gath.at[0, h], gath.at[0, h], 6, h1)
    attend(1)
    image_cross.wait_recv()
    image_relay = send(gath.at[0, h2], gath.at[0, h2], 7, h1)
    image_pair.wait_recv()
    image_relay.wait_recv()
    project(0)

    def spread(source, target, send_sem, recv_sem):
        copies = []
        for j in range(1, n):
            peer = lax.rem(me + j, n)
            copy = pltpu.make_async_remote_copy(
                src_ref=source(peer),
                dst_ref=target,
                send_sem=send_sem.at[j],
                recv_sem=recv_sem.at[j],
                device_id={"seq": peer},
            )
            copy.start()
            copies.append(copy)
        sent.extend(copies)
        return copies

    def piece(device):
        return pl.ds(pl.multiple_of(device * part, part), part)

    spans = spread(lambda peer: span_send, span_recv.at[me], span_send_sem, span_recv_sem)
    span_recv[me] = span_send[...]
    attend(0)
    states = spread(
        lambda peer: state.at[:, piece(peer)], state_recv.at[me], state_send_sem, state_recv_sem
    )
    keep_state = pltpu.make_async_copy(state.at[:, piece(me)], state_recv.at[me], keep_sem.at[0])
    keep_state.start()

    for copy in spans:
        copy.wait_recv()
    units = SPAN_ROWS * n
    my_head = (me * part) // LANES
    table = span_recv[...].reshape(units, LANES)
    span_col = jnp.sum(
        jnp.where(iota(table.shape, 1) == my_head, table, 0.0), axis=1, keepdims=True
    )
    eye = iota((units, units), 0) == iota((units, units), 1)
    span_row = jnp.sum(jnp.where(eye, span_col, 0.0), axis=0, keepdims=True)
    place_row, place_col = place_row_ref[...], place_col_ref[...]
    earlier = place_row < place_col
    later = place_col < place_row
    begin_col = jnp.sum(jnp.where(earlier, span_row, 0.0), axis=1, keepdims=True)
    begin_row = jnp.sum(jnp.where(later, span_col, 0.0), axis=0, keepdims=True)
    passed = jnp.minimum(begin_col - begin_row - span_row, 0.0)
    share = jnp.where(earlier, jnp.exp(passed), 0.0)
    share_high = share.astype(BF16)
    share_low = (share - share_high.astype(F32)).astype(BF16)
    total = 2 * n * part

    def unit_of(index):
        return index // (2 * part) * SPAN_ROWS + (index // part) % 2

    tall = (unit_of(iota((total, units), 0)) == iota((total, units), 1)).astype(BF16)
    wide = (unit_of(iota((units, total), 1)) == iota((units, total), 0)).astype(BF16)
    same = iota((total, total), 0) % part == iota((total, total), 1) % part

    def expand(values):
        grid = dot(dot(tall, values).astype(BF16), wide)
        return jnp.where(same, grid, 0.0).astype(BF16)

    mix_high = expand(share_high)
    mix_low = expand(share_low)
    keep_state.wait()
    for copy in states:
        copy.wait_recv()
    every = state_recv[...].reshape(total, LANES)
    joined = dot(mix_high, every) + dot(mix_low, every)
    entering_send[...] = joined.astype(BF16).reshape(n, 2, part, LANES)
    enters = spread(
        lambda peer: entering_send.at[peer],
        entering.at[:, piece(me)],
        enter_send_sem,
        enter_recv_sem,
    )
    keep_enter = pltpu.make_async_copy(
        entering_send.at[me], entering.at[:, piece(me)], keep_sem.at[1]
    )
    keep_enter.start()
    out_load.wait()
    keep_enter.wait()
    for copy in enters:
        copy.wait_recv()

    def finish(k):
        grown = jnp.exp(within_keep[k])
        pieces = []
        for i in range(heads):
            lane = slice(i * LANES, (i + 1) * LANES)
            carried = grown[:, i : i + 1] * dot(proj[k, 0, :, lane], entering[k, lane, :])
            attended = inner[k, :, lane] + carried
            mean_square = jnp.mean(attended * attended, axis=1, keepdims=True)
            unit = attended * lax.rsqrt(mean_square + EPSILON) * out_gain_ref[i : i + 1, :]
            gate = proj[k, 3, :, lane].astype(F32)
            pieces.append((unit * gate * jax.nn.sigmoid(gate)).astype(BF16))
        gated = jnp.concatenate(pieces, axis=1)
        out_send[k, 0] = dot(gated, w_out[:, columns(h3)]).astype(BF16)
        out_send[k, 1] = dot(gated, w_out[:, columns(h1)]).astype(BF16)
        copy = send(out_send.at[k], out_recv.at[k], 8 + k, h1)
        distant = dot(gated, w_out[:, columns(h2)])
        out_own[k] = dot(gated, w_out[:, columns(h)])
        copy.wait_recv()
        out_cross_send[k] = (distant + out_recv[k, 0].astype(F32)).astype(BF16)
        return send(out_cross_send.at[k], out_cross_recv.at[k], 10 + k, h2)

    def result(k):
        total_out = out_own[k] + out_recv[k, 1].astype(F32) + out_cross_recv[k].astype(F32)
        return (gath[k, h].astype(F32) + total_out).astype(BF16)

    first = finish(0)
    second = finish(1)
    first.wait_recv()
    image_out_ref[0] = result(0)
    second.wait_recv()
    text_out_ref[...] = result(1)
    for copy in sent:
        copy.wait_send()


def shards(
    image_patches,
    text_embed,
    image_start,
    image_forget,
    adapter,
    norm_gain,
    in_proj,
    decay_proj,
    head_decay_ceiling,
    out_gain,
    out_proj,
):
    n = lax.axis_size("seq")
    me = lax.axis_index("seq")
    rows, width = text_embed.shape
    model_width = in_proj.shape[0]
    heads = head_decay_ceiling.shape[0]
    part = heads * LANES // n
    places = unit_places(image_start, n)
    places = jnp.pad(places, ((0, 0), (0, SPAN_ROWS - 2)), constant_values=0).reshape(-1)
    used = jnp.arange(SPAN_ROWS * n) % SPAN_ROWS < 2
    place_row = jnp.where(used, places, 4 * n)[None, :]
    place_col = jnp.where(used, places, 4 * n)[:, None]
    burst = jnp.log1p(-lax.dynamic_index_in_dim(image_forget, me, 0, True))
    burst = jnp.broadcast_to(burst[None, :], (1, LANES))
    decay_pad = jnp.pad(decay_proj, ((0, 0), (0, LANES - heads)))
    ceiling = jnp.pad(head_decay_ceiling, (0, LANES - heads))[None, :]
    vmem = pl.BlockSpec(memory_space=pltpu.VMEM)
    hbm = pl.BlockSpec(memory_space=pl.ANY)
    dma = pltpu.SemaphoreType.DMA
    return pl.pallas_call(
        functools.partial(layer_kernel, n, heads),
        out_shape=(
            jax.ShapeDtypeStruct((1, rows, width), BF16),
            jax.ShapeDtypeStruct((rows, width), BF16),
        ),
        in_specs=[vmem] * 10 + [hbm] * 2,
        out_specs=(vmem, vmem),
        scratch_shapes=[
            pltpu.VMEM((4 * model_width, width), BF16),
            pltpu.VMEM((width // LANES, 512, LANES), F32),
            pltpu.VMEM((4, model_width, width), BF16),
            pltpu.VMEM((width, model_width), BF16),
            pltpu.VMEM((2, 4, rows, width), BF16),
            pltpu.VMEM((rows, model_width), BF16),
            pltpu.VMEM((2, 4, rows, width), BF16),
            pltpu.VMEM((2, rows, width), F32),
            pltpu.VMEM((2, rows, LANES), F32),
            pltpu.VMEM((2, rows, width), BF16),
            pltpu.VMEM((2, rows, width), BF16),
            pltpu.VMEM((rows, width), F32),
            pltpu.VMEM((rows, width), BF16),
            pltpu.VMEM((rows, width), BF16),
            pltpu.VMEM((2, 2, rows, width), BF16),
            pltpu.VMEM((2, 2, rows, width), BF16),
            pltpu.VMEM((2, rows, width), BF16),
            pltpu.VMEM((2, rows, width), BF16),
            pltpu.VMEM((2, rows, width), F32),
            pltpu.VMEM((2, heads * LANES, LANES), BF16),
            pltpu.VMEM((n, 2, part, LANES), BF16),
            pltpu.VMEM((n, 2, part, LANES), BF16),
            pltpu.VMEM((2, heads * LANES, LANES), BF16),
            pltpu.VMEM((SPAN_ROWS, LANES), F32),
            pltpu.VMEM((n, SPAN_ROWS, LANES), F32),
            dma((2,)),
            dma((12,)),
            dma((12,)),
            dma((n,)),
            dma((n,)),
            dma((n,)),
            dma((n,)),
            dma((n,)),
            dma((n,)),
            dma((2,)),
        ],
        compiler_params=pltpu.CompilerParams(
            collective_id=0, has_side_effects=True, vmem_limit_bytes=60 * 1024 * 1024
        ),
    )(
        image_patches[0],
        text_embed,
        adapter,
        norm_gain[None, :],
        decay_pad,
        ceiling,
        burst,
        out_gain,
        place_row,
        place_col,
        in_proj,
        out_proj,
    )


def solution(mesh):
    in_specs = (
        P("seq", None, "head"),
        P("seq", "head"),
        P(),
        P(),
        P("head", None),
        P(),
        P(None, None, "head"),
        P(None, "head"),
        P("head"),
        P("head", None),
        P("head", None),
    )
    out_specs = (P("seq", None, "head"), P("seq", "head"))
    return jax.shard_map(shards, mesh=mesh, in_specs=in_specs, out_specs=out_specs, check_vma=False)
```
